128 devices in a mesh: py: 32 (over z_hi, y, x), px: 4 (over z_lo, core).
Axes of the slice: x: 4, y: 4, z: 4 (z_hi: 2, z_lo: 2; z = z_hi * 2 + z_lo), core: 2. Of those that a mesh axis runs over, the one named last changes fastest.
Arguments:
- source_terms: float32 [2048, 512, 256], P('py', 'px'), may hold values from -6 to 6
- initial_values: float32 [2048, 512, 256], P('py', 'px'), may hold values from -6 to 6
- absorption: float32 [2048, 512, 256], P('py', 'px'), may hold values from 0.1 to 0.9
Outputs:
- improved: float32 [2048, 512, 256], P('py', 'px')
The draws below stay inside these ranges and needn't reach their ends.
All inputs are finite; a program needn't handle non-finite values.
Results may differ from the reference program's by a relative error of at most 0.00002.
Values sent between devices are 32-bit elements; how exact they have to be, the bound alone decides.
A program may use at most 128 MiB of HBM per device.

```python
import jax
import jax.numpy as jnp
from jax import lax

CASES = 256
RATIO = 4
BEFORE = 2
AFTER = 2
INNER = 13
GRID_Y = 2048
GRID_X = 512


def block_scale(rng, extent, pieces, low, largest):
    level = 1.0
    for position, shards_of in pieces:
        steps = jax.random.uniform(jax.random.fold_in(jax.random.fold_in(rng, 6), position), (shards_of,), jnp.float32, low / len(pieces), largest / len(pieces))
        level = level * jnp.repeat(jnp.exp(steps), extent[position] // shards_of).reshape((-1,) + (1,) * (len(extent) - 1 - position))
    return level


def noise(key, dims, scale, limit, split=(), dtype=jnp.bfloat16):
    loudness = block_scale(key, dims, split, -0.22, 0.18) if split else 1.0
    drawn = jax.random.normal(key, dims, jnp.float32) * scale * loudness
    return jnp.minimum(jnp.maximum(drawn, -limit), limit).astype(dtype)


def setup_inputs(seed: int = 0) -> dict:
    keys = jax.random.split(jax.random.key(seed), 4)
    return {
        "source_terms": noise(keys[0], (GRID_Y, GRID_X, CASES), 1.0, 6.0, ((0, 32), (1, 4)), jnp.float32),
        "initial_values": noise(keys[1], (GRID_Y, GRID_X, CASES), 1.0, 6.0, ((0, 32), (1, 4)), jnp.float32),
        "absorption": jnp.clip(0.1 + 0.79999997 * jax.random.uniform(keys[2], (GRID_Y, GRID_X, CASES), jnp.float32) ** block_scale(keys[2], (GRID_Y, GRID_X, CASES), ((0, 32), (1, 4)), -0.2, 0.2), 0.1, 0.9),
    }


def around_sum(padded):
    inner_y, inner_x = padded.shape[0] - 2, padded.shape[1] - 2
    middle_rows = lax.slice_in_dim(padded, 1, 1 + inner_y, axis=0)
    middle_columns = lax.slice_in_dim(padded, 1, 1 + inner_x, axis=1)
    return (lax.slice_in_dim(middle_columns, 0, inner_y, axis=0) + lax.slice_in_dim(middle_columns, 2, 2 + inner_y, axis=0)
            + lax.slice_in_dim(middle_rows, 0, inner_x, axis=1) + lax.slice_in_dim(middle_rows, 2, 2 + inner_x, axis=1))


def relax_once(padded, values, load, mass_here):
    return values + 0.8 * (load + around_sum(padded) - (4.0 + mass_here) * values) / (4.0 + mass_here)


def block_means(values):
    cut = values.reshape(values.shape[0] // RATIO, RATIO, values.shape[1] // RATIO, RATIO, values.shape[2])
    return jnp.mean(cut, axis=(1, 3))


def spread_blocks(values):
    return jnp.repeat(jnp.repeat(values, RATIO, axis=0), RATIO, axis=1)


def reference(source_terms, initial_values, absorption):
    values = initial_values
    for sweep in range(BEFORE):
        values = relax_once(jnp.pad(values, ((1, 1), (1, 1), (0, 0)), mode="wrap"), values, source_terms, absorption)
    defect = source_terms + around_sum(jnp.pad(values, ((1, 1), (1, 1), (0, 0)), mode="wrap")) - (4.0 + absorption) * values
    coarse_load, coarse_mass = block_means(defect) * RATIO, block_means(absorption) * RATIO
    coarse_values = jnp.zeros_like(coarse_load)
    for sweep in range(INNER):
        coarse_values = relax_once(jnp.pad(coarse_values, ((1, 1), (1, 1), (0, 0)), mode="wrap"), coarse_values, coarse_load, coarse_mass)
    values = values + spread_blocks(coarse_values)
    for sweep in range(AFTER):
        values = relax_once(jnp.pad(values, ((1, 1), (1, 1), (0, 0)), mode="wrap"), values, source_terms, absorption)
    improved = values
    return improved
```

```python
import jax
import jax.numpy as jnp
from jax import lax
from jax.experimental import pallas as pl
from jax.experimental.pallas import tpu as pltpu
from jax.sharding import PartitionSpec as P

MESH = pl.DeviceIdType.MESH
RATIO = 4
INNER = 13
DEPTH = 13
PX = 8
CPX = 16


def coarse_pieces(rows, cols):
    early, late = [], []
    last = rows - 1
    early.append((-1, 0, 1, DEPTH - 1, 0, cols))
    early.append((1, 0, rows - DEPTH, DEPTH - 1, 0, cols))
    for dx in (-1, 1):
        wide = 0 if dx < 0 else cols - 16
        thin = 0 if dx < 0 else cols - 8
        early.append((0, dx, 1, rows - 2, wide, 16))
        early.append((-1, dx, 1, 3, wide, 16))
        early.append((-1, dx, 4, 8, thin, 8))
        early.append((1, dx, last - 3, 3, wide, 16))
        early.append((1, dx, last - 11, 8, thin, 8))
    late.append((-1, 0, 0, 1, 0, cols))
    late.append((1, 0, last, 1, 0, cols))
    for dx in (-1, 1):
        wide = 0 if dx < 0 else cols - 16
        late.append((-1, dx, 0, 1, wide, 16))
        late.append((1, dx, last, 1, wide, 16))
        late.append((0, dx, 0, 1, wide, 16))
        late.append((0, dx, last, 1, wide, 16))
    return early, late


def kernel(ny, nx, source, initial, absorb, out,
           U, V, S, D, W, CL, CW, CA, CB, E, T, LY, LX, KX,
           ld_sem, out_sem, ys, yr, xs, xr, cs, cr):
    J, Y, X = S.shape[0], S.shape[1], S.shape[2]
    CY, CX = Y // RATIO, X // RATIO
    my, mx = lax.axis_index("py"), lax.axis_index("px")

    def device(dy, dx):
        return (lax.rem(my + dy + ny, ny), lax.rem(mx + dx + nx, nx))

    chunks = 4
    step = Y // chunks

    def loads(array, which, ref, padded):
        made = []
        for c in range(chunks):
            for j in range(J):
                if padded:
                    dst = ref.at[j, pl.ds(1 + c * step, step), pl.ds(PX, X), :]
                else:
                    dst = ref.at[j, pl.ds(c * step, step), :, :]
                made.append(pltpu.make_async_copy(
                    array.at[pl.ds(c * step, step), :, pl.ds(j * 128, 128)], dst, ld_sem.at[which, c * J + j]))
        return made

    load_u = loads(initial, 0, U, True)
    load_d = loads(absorb, 1, D, False)
    load_s = loads(source, 2, S, False)
    for copy in load_u + load_d + load_s:
        copy.start()

    around = [(dy, dx) for dy in (-1, 0, 1) for dx in (-1, 0, 1) if (dy, dx) != (0, 0)]
    barrier = pltpu.get_barrier_semaphore()
    for dy, dx in around:
        pl.semaphore_signal(barrier, inc=1, device_id=device(dy, dx), device_id_type=MESH)
    pl.semaphore_wait(barrier, len(around))

    def rows_copies(k, ref):
        return [
            pltpu.make_async_remote_copy(
                src_ref=ref.at[:, 1, pl.ds(PX, X), :], dst_ref=LY.at[k, 1], send_sem=ys.at[k, 1], recv_sem=yr.at[k, 1],
                device_id=device(-1, 0), device_id_type=MESH),
            pltpu.make_async_remote_copy(
                src_ref=ref.at[:, Y, pl.ds(PX, X), :], dst_ref=LY.at[k, 0], send_sem=ys.at[k, 0], recv_sem=yr.at[k, 0],
                device_id=device(1, 0), device_id_type=MESH),
        ]

    def columns_copies(k):
        return [
            pltpu.make_async_remote_copy(
                src_ref=KX.at[k, 1], dst_ref=LX.at[k, 1], send_sem=xs.at[k, 1], recv_sem=xr.at[k, 1],
                device_id=device(0, -1), device_id_type=MESH),
            pltpu.make_async_remote_copy(
                src_ref=KX.at[k, 0], dst_ref=LX.at[k, 0], send_sem=xs.at[k, 0], recv_sem=xr.at[k, 0],
                device_id=device(0, 1), device_id_type=MESH),
        ]

    def start(copies):
        for copy in copies:
            copy.start()

    def received(copies):
        for copy in copies:
            copy.wait_recv()

    def sent(copies):
        for copy in copies:
            copy.wait_send()

    def pack(k, ref):
        def body(y, carry):
            for j in range(J):
                KX[k, 1, j, pl.ds(y, 1), :] = ref[j, y + 1, pl.ds(PX, 1), :]
                KX[k, 0, j, pl.ds(y, 1), :] = ref[j, y + 1, pl.ds(PX + X - 1, 1), :]
            return carry
        lax.fori_loop(0, Y, body, 0)

    def unpack_columns(k, ref):
        def body(y, carry):
            for j in range(J):
                ref[j, y + 1, pl.ds(PX + X, 1), :] = LX[k, 1, j, pl.ds(y, 1), :]
                ref[j, y + 1, pl.ds(PX - 1, 1), :] = LX[k, 0, j, pl.ds(y, 1), :]
            return carry
        lax.fori_loop(0, Y, body, 0)

    def unpack_rows(k, ref):
        for j in range(J):
            ref[j, 0, pl.ds(PX, X), :] = LY[k, 0, j]
            ref[j, Y + 1, pl.ds(PX, X), :] = LY[k, 1, j]

    def neighbours(ref, j, y):
        return (ref[j, y, pl.ds(PX, X), :] + ref[j, y + 2, pl.ds(PX, X), :]
                + (ref[j, y + 1, pl.ds(PX - 1, X), :] + ref[j, y + 1, pl.ds(PX + 1, X), :]))

    def sweep_row(src, dst, y):
        for j in range(J):
            total = S[j, y] + neighbours(src, j, y)
            dst[j, y + 1, pl.ds(PX, X), :] = 0.2 * src[j, y + 1, pl.ds(PX, X), :] + W[j, y] * total

    def inner_rows(src, dst, low, high):
        def body(y, carry):
            sweep_row(src, dst, y)
            return carry
        lax.fori_loop(low, high, body, 0)

    def outer_rows(src, dst):
        def body(i, carry):
            sweep_row(src, dst, i * (Y - 1))
            return carry
        lax.fori_loop(0, 2, body, 0)

    early, late = coarse_pieces(CY, CX)

    def coarse_copies(ref, pieces, base):
        made = []
        for n, (dy, dx, r, nr, c, nc) in enumerate(pieces):
            made.append(pltpu.make_async_remote_copy(
                src_ref=ref.at[:, pl.ds(DEPTH + r, nr), pl.ds(CPX + c, nc), :],
                dst_ref=ref.at[:, pl.ds(DEPTH + r - CY * dy, nr), pl.ds(CPX + c - CX * dx, nc), :],
                send_sem=cs.at[base + n], recv_sem=cr.at[base + n],
                device_id=device(dy, dx), device_id_type=MESH))
        return made

    n_early, n_late = len(early), len(late)
    mass_copies = coarse_copies(CW, early + late, 0)
    load_early = coarse_copies(CL, early, n_early + n_late)
    load_late = coarse_copies(CL, late, 2 * n_early + n_late)

    rows0, rows1, rows2, rows3 = (rows_copies(0, U), rows_copies(1, V), rows_copies(2, U), rows_copies(3, V))
    cols0, cols1, cols2, cols3 = (columns_copies(0), columns_copies(1), columns_copies(2), columns_copies(3))
    for copy in load_u:
        copy.wait()
    start(rows0)
    pack(0, U)
    start(cols0)

    for copy in load_d:
        copy.wait()

    def weight_row(cy, carry):
        for j in range(J):
            total = jnp.zeros((X, 128), jnp.float32)
            for r in range(RATIO):
                mass = D[j, cy * RATIO + r]
                total = total + mass
                whole = 4.0 + mass
                D[j, cy * RATIO + r] = whole
                W[j, cy * RATIO + r] = 0.8 / whole
            T[j] = total
            blocks = (T[j, pl.ds(0, CX, stride=RATIO), :] + T[j, pl.ds(1, CX, stride=RATIO), :]
                      + T[j, pl.ds(2, CX, stride=RATIO), :] + T[j, pl.ds(3, CX, stride=RATIO), :])
            CW[j, DEPTH + cy, pl.ds(CPX, CX), :] = 0.8 / (4.0 + 0.25 * blocks)
        return carry
    lax.fori_loop(0, CY, weight_row, 0)

    for copy in load_s:
        copy.wait()
    received(cols0)
    unpack_columns(0, U)
    inner_rows(U, V, 1, Y - 1)
    received(rows0)
    unpack_rows(0, U)
    outer_rows(U, V)
    start(rows1)
    pack(1, V)
    start(cols1)
    start(mass_copies)

    sent(rows0)
    received(cols1)
    unpack_columns(1, V)
    inner_rows(V, U, 1, Y - 1)
    received(rows1)
    unpack_rows(1, V)
    outer_rows(V, U)
    start(rows2)
    pack(2, U)
    start(cols2)

    def defect_row(cy):
        for j in range(J):
            total = jnp.zeros((X, 128), jnp.float32)
            for r in range(RATIO):
                y = cy * RATIO + r
                total = total + (S[j, y] + neighbours(U, j, y) - D[j, y] * U[j, y + 1, pl.ds(PX, X), :])
            T[j] = total
            blocks = (T[j, pl.ds(0, CX, stride=RATIO), :] + T[j, pl.ds(1, CX, stride=RATIO), :]
                      + T[j, pl.ds(2, CX, stride=RATIO), :] + T[j, pl.ds(3, CX, stride=RATIO), :])
            CL[j, DEPTH + cy, pl.ds(CPX, CX), :] = 0.25 * blocks

    def defect_body(cy, carry):
        defect_row(cy)
        return carry

    def defect_ends(i, carry):
        defect_row(i * (CY - 1))
        return carry

    received(cols2)
    unpack_columns(2, U)
    lax.fori_loop(1, CY - 1, defect_body, 0)
    start(load_early)
    received(rows2)
    unpack_rows(2, U)
    lax.fori_loop(0, 2, defect_ends, 0)
    start(load_late)
    received(mass_copies)
    received(load_early)
    received(load_late)

    wide = CX + 2 * CPX

    def first(y, carry):
        for j in range(J):
            CA[j, y] = CW[j, y] * CL[j, y]
        return carry
    lax.fori_loop(0, CY + 2 * DEPTH, first, 0)
    old, new = CA, CB
    for sweep in range(1, INNER):
        reach = DEPTH - sweep
        x0 = 8 if reach <= 8 else 1
        nx_ = CX + 2 * (CPX - x0)

        def coarse_row(y, carry, old=old, new=new, x0=x0, nx_=nx_):
            for j in range(J):
                total = (CL[j, y, pl.ds(x0, nx_), :] + old[j, y - 1, pl.ds(x0, nx_), :] + old[j, y + 1, pl.ds(x0, nx_), :]
                         + (old[j, y, pl.ds(x0 - 1, nx_), :] + old[j, y, pl.ds(x0 + 1, nx_), :]))
                new[j, y, pl.ds(x0, nx_), :] = 0.2 * old[j, y, pl.ds(x0, nx_), :] + CW[j, y, pl.ds(x0, nx_), :] * total
            return carry
        lax.fori_loop(DEPTH - reach, DEPTH + CY + reach, coarse_row, 0)
        old, new = new, old
    C = old

    def spread(cy):
        for j in range(J):
            cells = C[j, DEPTH + cy, pl.ds(CPX, CX), :]
            for k in range(RATIO):
                E[j, pl.ds(PX + k, CX, stride=RATIO), :] = cells
            E[j, pl.ds(PX - 1, 1), :] = C[j, DEPTH + cy, pl.ds(CPX - 1, 1), :]
            E[j, pl.ds(PX + X, 1), :] = C[j, DEPTH + cy, pl.ds(CPX + CX, 1), :]

    def add_row(y):
        for j in range(J):
            U[j, y] = U[j, y] + E[j]

    sent(rows2)

    def correct(cy, carry):
        spread(cy)
        for r in range(RATIO):
            add_row(1 + cy * RATIO + r)
        return carry

    spread(-1)
    add_row(0)
    lax.fori_loop(0, CY, correct, 0)
    spread(CY)
    add_row(Y + 1)

    sent(rows1)
    outer_rows(U, V)
    start(rows3)
    inner_rows(U, V, 1, Y - 1)
    pack(3, V)
    start(cols3)
    received(cols3)
    unpack_columns(3, V)

    def stores(low, count, sem):
        return [pltpu.make_async_copy(
            U.at[j, pl.ds(1 + low, count), pl.ds(PX, X), :], out.at[pl.ds(low, count), :, pl.ds(j * 128, 128)],
            out_sem.at[sem, j]) for j in range(J)]

    pending = []
    bounds = [1, 16, 32, 48, Y - 1]
    for n in range(4):
        inner_rows(V, U, bounds[n], bounds[n + 1])
        copies = stores(bounds[n], bounds[n + 1] - bounds[n], n)
        start(copies)
        pending += copies
    received(rows3)
    unpack_rows(3, V)
    outer_rows(V, U)
    for n, y in ((4, 0), (5, Y - 1)):
        copies = stores(y, 1, n)
        start(copies)
        pending += copies
    for copy in pending:
        copy.wait()
    sent(rows3)
    for copies in (cols0, cols1, cols2, cols3, mass_copies, load_early, load_late):
        sent(copies)


def solution(mesh):
    ny, nx = mesh.shape["py"], mesh.shape["px"]

    def local(source_terms, initial_values, absorption):
        Y, X, cases = source_terms.shape
        J = cases // 128
        CY, CX = Y // RATIO, X // RATIO
        early, late = coarse_pieces(CY, CX)
        pieces = 2 * (len(early) + len(late))
        f32 = jnp.float32
        fine = pltpu.VMEM((J, Y + 2, X + 2 * PX, 128), f32)
        plain = pltpu.VMEM((J, Y, X, 128), f32)
        coarse = pltpu.VMEM((J, CY + 2 * DEPTH, CX + 2 * CPX, 128), f32)
        dma = pltpu.SemaphoreType.DMA

        def body(*refs):
            kernel(ny, nx, *refs)

        return pl.pallas_call(
            body,
            out_shape=jax.ShapeDtypeStruct((Y, X, cases), f32),
            in_specs=[pl.BlockSpec(memory_space=pl.ANY)] * 3,
            out_specs=pl.BlockSpec(memory_space=pl.ANY),
            scratch_shapes=[
                fine, fine, plain, plain, plain, coarse, coarse, coarse, coarse,
                pltpu.VMEM((J, X + 2 * PX, 128), f32),
                pltpu.VMEM((J, X, 128), f32),
                pltpu.VMEM((4, 2, J, X, 128), f32),
                pltpu.VMEM((4, 2, J, Y, 128), f32),
                pltpu.VMEM((4, 2, J, Y, 128), f32),
                dma((3, 4 * J)), dma((6, J)),
                dma((4, 2)), dma((4, 2)), dma((4, 2)), dma((4, 2)),
                dma((pieces,)), dma((pieces,)),
            ],
            compiler_params=pltpu.CompilerParams(
                collective_id=0, has_side_effects=True, vmem_limit_bytes=67043328),
            name="two_grid",
        )(source_terms, initial_values, absorption)

    spec = P("py", "px", None)
    return jax.shard_map(local, mesh=mesh, in_specs=(spec, spec, spec), out_specs=spec, check_vma=False)
```

```python
import jax
import jax.numpy as jnp
from jax import lax
from jax.experimental import pallas as pl
from jax.experimental.pallas import tpu as pltpu
from jax.sharding import PartitionSpec as P

MESH = pl.DeviceIdType.MESH
RATIO = 4
INNER = 13
DEPTH = 6
AGAIN = 7
PX = 8
CPX = 16


def coarse_pieces(depth, rows, cols, part):
    first, last = (0, rows) if part == "all" else (1, rows - 1)
    spans = []
    if part == "late":
        spans += [(-1, 0, 1), (1, rows - 1, 1)]
    else:
        spans += [(-1, first, depth - first), (1, rows - depth, last - (rows - depth))]
    made = [(dy, 0, r, n, 0, cols) for dy, r, n in spans]
    for dx in (-1, 1):
        c = 0 if dx < 0 else cols - 8
        if part == "late":
            made += [(0, dx, 0, 1, c, 8), (0, dx, rows - 1, 1, c, 8), (-1, dx, 0, 1, c, 8), (1, dx, rows - 1, 1, c, 8)]
        else:
            made += [(0, dx, first, last - first, c, 8), (-1, dx, first, depth - 1 - first, c, 8),
                     (1, dx, rows - depth + 1, last - (rows - depth + 1), c, 8)]
    return made


def kernel(ny, nx, source, initial, absorb, D,
           U, V, S, W, CL, CW, CA, CB, CC, E, T, LY, LX, KX,
           ld_sem, ys, yr, xs, xr, cs, cr):
    J, Y, X = S.shape[0], S.shape[1], S.shape[2]
    CY, CX = Y // RATIO, X // RATIO
    my, mx = lax.axis_index("py"), lax.axis_index("px")

    def device(dy, dx):
        return (lax.rem(my + dy + ny, ny), lax.rem(mx + dx + nx, nx))

    chunks = 4
    step = Y // chunks

    def loads(array, which, ref, padded):
        made = []
        for c in range(chunks):
            for j in range(J):
                if padded:
                    dst = ref.at[j, pl.ds(1 + c * step, step), pl.ds(PX, X), :]
                else:
                    dst = ref.at[j, pl.ds(c * step, step), :, :]
                made.append(pltpu.make_async_copy(
                    array.at[pl.ds(c * step, step), :, pl.ds(j * 128, 128)], dst, ld_sem.at[which, c * J + j]))
        return made

    load_u = loads(initial, 0, U, True)
    load_d = loads(absorb, 1, D, False)
    load_s = loads(source, 2, S, False)
    for copy in load_u + load_d + load_s:
        copy.start()

    around = [(dy, dx) for dy in (-1, 0, 1) for dx in (-1, 0, 1) if (dy, dx) != (0, 0)]
    barrier = pltpu.get_barrier_semaphore()
    for dy, dx in around:
        pl.semaphore_signal(barrier, inc=1, device_id=device(dy, dx), device_id_type=MESH)
    with jax.named_scope("barrier"):
        pl.semaphore_wait(barrier, len(around))

    def rows_copies(k, ref):
        return [
            pltpu.make_async_remote_copy(
                src_ref=ref.at[:, 1, pl.ds(PX, X), :], dst_ref=LY.at[k, 1], send_sem=ys.at[k, 1], recv_sem=yr.at[k, 1],
                device_id=device(-1, 0), device_id_type=MESH),
            pltpu.make_async_remote_copy(
                src_ref=ref.at[:, Y, pl.ds(PX, X), :], dst_ref=LY.at[k, 0], send_sem=ys.at[k, 0], recv_sem=yr.at[k, 0],
                device_id=device(1, 0), device_id_type=MESH),
        ]

    def columns_copies(k):
        return [
            pltpu.make_async_remote_copy(
                src_ref=KX.at[k, 1], dst_ref=LX.at[k, 1], send_sem=xs.at[k, 1], recv_sem=xr.at[k, 1],
                device_id=device(0, -1), device_id_type=MESH),
            pltpu.make_async_remote_copy(
                src_ref=KX.at[k, 0], dst_ref=LX.at[k, 0], send_sem=xs.at[k, 0], recv_sem=xr.at[k, 0],
                device_id=device(0, 1), device_id_type=MESH),
        ]

    def start(copies):
        for copy in copies:
            copy.start()

    def received(copies):
        for copy in copies:
            copy.wait_recv()

    def sent(copies):
        for copy in copies:
            copy.wait_send()

    def pack(k, ref):
        def body(y, carry):
            for j in range(J):
                KX[k, 1, j, pl.ds(y, 1), :] = ref[j, y + 1, pl.ds(PX, 1), :]
                KX[k, 0, j, pl.ds(y, 1), :] = ref[j, y + 1, pl.ds(PX + X - 1, 1), :]
            return carry
        lax.fori_loop(0, Y, body, 0)

    def unpack_columns(k, ref):
        def body(y, carry):
            for j in range(J):
                ref[j, y + 1, pl.ds(PX + X, 1), :] = LX[k, 1, j, pl.ds(y, 1), :]
                ref[j, y + 1, pl.ds(PX - 1, 1), :] = LX[k, 0, j, pl.ds(y, 1), :]
            return carry
        lax.fori_loop(0, Y, body, 0)

    def unpack_rows(k, ref):
        for j in range(J):
            ref[j, 0, pl.ds(PX, X), :] = LY[k, 0, j]
            ref[j, Y + 1, pl.ds(PX, X), :] = LY[k, 1, j]

    def neighbours(ref, j, y):
        return (ref[j, y, pl.ds(PX, X), :] + ref[j, y + 2, pl.ds(PX, X), :]
                + (ref[j, y + 1, pl.ds(PX - 1, X), :] + ref[j, y + 1, pl.ds(PX + 1, X), :]))

    def sweep_row(src, dst, y):
        for j in range(J):
            total = S[j, y] + neighbours(src, j, y)
            dst[j, y + 1, pl.ds(PX, X), :] = 0.2 * src[j, y + 1, pl.ds(PX, X), :] + W[j, y] * total

    def inner_rows(src, dst, low, high):
        def body(y, carry):
            sweep_row(src, dst, y)
            return carry
        lax.fori_loop(low, high, body, 0)

    def outer_rows(src, dst):
        def body(i, carry):
            sweep_row(src, dst, i * (Y - 1))
            return carry
        lax.fori_loop(0, 2, body, 0)

    def coarse_copies(ref, depth, part, base):
        made = []
        for n, (dy, dx, r, nr, c, nc) in enumerate(coarse_pieces(depth, CY, CX, part)):
            made.append(pltpu.make_async_remote_copy(
                src_ref=ref.at[:, pl.ds(AGAIN + r, nr), pl.ds(CPX + c, nc), :],
                dst_ref=ref.at[:, pl.ds(AGAIN + r - CY * dy, nr), pl.ds(CPX + c - CX * dx, nc), :],
                send_sem=cs.at[base + n], recv_sem=cr.at[base + n],
                device_id=device(dy, dx), device_id_type=MESH))
        return made

    mass_copies = coarse_copies(CW, DEPTH, "all", 0)
    load_early = coarse_copies(CL, DEPTH, "early", 8)
    load_late = coarse_copies(CL, DEPTH, "late", 16)
    value_copies = coarse_copies(CC, AGAIN, "all", 26)

    rows0, rows1, rows2, rows3 = (rows_copies(0, U), rows_copies(1, V), rows_copies(2, U), rows_copies(3, V))
    cols0, cols1, cols2, cols3 = (columns_copies(0), columns_copies(1), columns_copies(2), columns_copies(3))
    with jax.named_scope("wait_u"):
        for copy in load_u:
            copy.wait()
    with jax.named_scope("pack0"):
        start(rows0)
        pack(0, U)
        start(cols0)

    with jax.named_scope("wait_d"):
        for copy in load_d:
            copy.wait()

    def weight_row(cy, carry):
        for j in range(J):
            total = jnp.zeros((X, 128), jnp.float32)
            for r in range(RATIO):
                mass = D[j, cy * RATIO + r]
                total = total + mass
                whole = 4.0 + mass
                D[j, cy * RATIO + r] = whole
                W[j, cy * RATIO + r] = 0.8 / whole
            T[j] = total
            blocks = (T[j, pl.ds(0, CX, stride=RATIO), :] + T[j, pl.ds(1, CX, stride=RATIO), :]
                      + T[j, pl.ds(2, CX, stride=RATIO), :] + T[j, pl.ds(3, CX, stride=RATIO), :])
            CW[j, AGAIN + cy, pl.ds(CPX, CX), :] = 0.8 / (4.0 + 0.25 * blocks)
        return carry
    with jax.named_scope("weights"):
        lax.fori_loop(0, CY, weight_row, 0)
        start(mass_copies)

    with jax.named_scope("wait_s_x0"):
        for copy in load_s:
            copy.wait()
        received(cols0)
    with jax.named_scope("sweep1"):
        unpack_columns(0, U)
        inner_rows(U, V, 1, Y - 1)
    with jax.named_scope("wait_y0"):
        received(rows0)
    with jax.named_scope("outer1"):
        unpack_rows(0, U)
        outer_rows(U, V)
        start(rows1)
        pack(1, V)
        start(cols1)

    with jax.named_scope("wait_x1"):
        sent(rows0)
        received(cols1)
    with jax.named_scope("sweep2"):
        unpack_columns(1, V)
        inner_rows(V, U, 1, Y - 1)
    with jax.named_scope("wait_y1"):
        received(rows1)
    with jax.named_scope("outer2"):
        unpack_rows(1, V)
        outer_rows(V, U)
        start(rows2)
        pack(2, U)
        start(cols2)

    def defect_row(cy):
        for j in range(J):
            total = jnp.zeros((X, 128), jnp.float32)
            for r in range(RATIO):
                y = cy * RATIO + r
                total = total + (S[j, y] + neighbours(U, j, y) - D[j, y] * U[j, y + 1, pl.ds(PX, X), :])
            T[j] = total
            blocks = (T[j, pl.ds(0, CX, stride=RATIO), :] + T[j, pl.ds(1, CX, stride=RATIO), :]
                      + T[j, pl.ds(2, CX, stride=RATIO), :] + T[j, pl.ds(3, CX, stride=RATIO), :])
            CL[j, AGAIN + cy, pl.ds(CPX, CX), :] = 0.25 * blocks

    def defect_body(cy, carry):
        defect_row(cy)
        return carry

    def defect_ends(i, carry):
        defect_row(i * (CY - 1))
        return carry

    with jax.named_scope("wait_x2"):
        received(cols2)
    with jax.named_scope("defect"):
        unpack_columns(2, U)
        lax.fori_loop(1, CY - 1, defect_body, 0)
        start(load_early)
    with jax.named_scope("wait_y2"):
        received(rows2)
    with jax.named_scope("defect_ends"):
        unpack_rows(2, U)
        lax.fori_loop(0, 2, defect_ends, 0)
        start(load_late)
    with jax.named_scope("wait_mass"):
        received(mass_copies)
    with jax.named_scope("wait_load"):
        received(load_early)
        received(load_late)

    def first(y, carry):
        for j in range(J):
            CA[j, y] = CW[j, y] * CL[j, y]
        return carry

    def coarse_sweep(old, new, reach):
        x0 = CPX - 8 if reach > 0 else CPX
        wide = CX + 2 * (CPX - x0)

        def coarse_row(y, carry):
            for j in range(J):
                total = (CL[j, y, pl.ds(x0, wide), :] + old[j, y - 1, pl.ds(x0, wide), :] + old[j, y + 1, pl.ds(x0, wide), :]
                         + (old[j, y, pl.ds(x0 - 1, wide), :] + old[j, y, pl.ds(x0 + 1, wide), :]))
                new[j, y, pl.ds(x0, wide), :] = 0.2 * old[j, y, pl.ds(x0, wide), :] + CW[j, y, pl.ds(x0, wide), :] * total
            return carry
        lax.fori_loop(AGAIN - reach, AGAIN + CY + reach, coarse_row, 0)

    with jax.named_scope("coarse1"):
        lax.fori_loop(AGAIN - DEPTH, AGAIN + CY + DEPTH, first, 0)
        old, new = CA, CB
        for reach in range(DEPTH - 1, -1, -1):
            coarse_sweep(old, CC if reach == 0 else new, reach)
            old, new = new, old
        start(value_copies)
    with jax.named_scope("wait_value"):
        received(value_copies)
    with jax.named_scope("coarse2"):
        old, new = CC, CA
        for reach in range(AGAIN - 1, 0, -1):
            coarse_sweep(old, new, reach)
            old, new = new, (CB if new is CA else CA)
        C = old

    def spread(cy):
        for j in range(J):
            cells = C[j, AGAIN + cy, pl.ds(CPX, CX), :]
            for k in range(RATIO):
                E[j, pl.ds(PX + k, CX, stride=RATIO), :] = cells
            E[j, pl.ds(PX - 1, 1), :] = C[j, AGAIN + cy, pl.ds(CPX - 1, 1), :]
            E[j, pl.ds(PX + X, 1), :] = C[j, AGAIN + cy, pl.ds(CPX + CX, 1), :]

    def add_row(y):
        for j in range(J):
            U[j, y] = U[j, y] + E[j]

    sent(rows2)

    def correct(cy, carry):
        spread(cy)
        for r in range(RATIO):
            add_row(1 + cy * RATIO + r)
        return carry

    spread(-1)
    add_row(0)
    with jax.named_scope("correct"):
        lax.fori_loop(0, CY, correct, 0)
        spread(CY)
        add_row(Y + 1)

    sent(rows1)
    with jax.named_scope("sweep3"):
        outer_rows(U, V)
        start(rows3)
        inner_rows(U, V, 1, Y - 1)
        pack(3, V)
        start(cols3)
    with jax.named_scope("wait_x3"):
        received(cols3)
    unpack_columns(3, V)

    def last_row(y, carry):
        for j in range(J):
            total = S[j, y] + neighbours(V, j, y)
            D[j, y] = 0.2 * V[j, y + 1, pl.ds(PX, X), :] + W[j, y] * total
        return carry

    with jax.named_scope("sweep4"):
        lax.fori_loop(1, Y - 1, last_row, 0)
    with jax.named_scope("wait_y3"):
        received(rows3)
    with jax.named_scope("outer4"):
        unpack_rows(3, V)
        lax.fori_loop(0, 2, lambda i, carry: last_row(i * (Y - 1), carry), 0)
    sent(rows3)
    for copies in (cols0, cols1, cols2, cols3, mass_copies, load_early, load_late, value_copies):
        sent(copies)


def store(held, out, sems):
    J, Y, X = held.shape[0], held.shape[1], held.shape[2]
    copies = []
    for n in range(4):
        for j in range(J):
            rows = pl.ds(n * Y // 4, Y // 4)
            copies.append(pltpu.make_async_copy(held.at[j, rows], out.at[rows, :, pl.ds(j * 128, 128)], sems.at[n, j]))
    for copy in copies:
        copy.start()
    for copy in copies:
        copy.wait()


def solution(mesh):
    ny, nx = mesh.shape["py"], mesh.shape["px"]

    def local(source_terms, initial_values, absorption):
        Y, X, cases = source_terms.shape
        J = cases // 128
        CY, CX = Y // RATIO, X // RATIO
        f32 = jnp.float32
        fine = pltpu.VMEM((J, Y + 2, X + 2 * PX, 128), f32)
        plain = pltpu.VMEM((J, Y, X, 128), f32)
        coarse = pltpu.VMEM((J, CY + 2 * AGAIN, CX + 2 * CPX, 128), f32)
        dma = pltpu.SemaphoreType.DMA

        def body(*refs):
            kernel(ny, nx, *refs)

        held = pl.pallas_call(
            body,
            out_shape=plain,
            in_specs=[pl.BlockSpec(memory_space=pl.ANY)] * 3,
            out_specs=pl.BlockSpec(memory_space=pltpu.VMEM),
            scratch_shapes=[
                fine, fine, plain, plain, coarse, coarse, coarse, coarse, coarse,
                pltpu.VMEM((J, X + 2 * PX, 128), f32),
                pltpu.VMEM((J, X, 128), f32),
                pltpu.VMEM((4, 2, J, X, 128), f32),
                pltpu.VMEM((4, 2, J, Y, 128), f32),
                pltpu.VMEM((4, 2, J, Y, 128), f32),
                dma((3, 4 * J)),
                dma((4, 2)), dma((4, 2)), dma((4, 2)), dma((4, 2)),
                dma((34,)), dma((34,)),
            ],
            compiler_params=pltpu.CompilerParams(
                collective_id=0, has_side_effects=True, vmem_limit_bytes=50 * 1024 * 1024),
            name="two_grid",
        )(source_terms, initial_values, absorption)
        return pl.pallas_call(
            store,
            out_shape=jax.ShapeDtypeStruct((Y, X, cases), f32),
            in_specs=[pl.BlockSpec(memory_space=pltpu.VMEM)],
            out_specs=pl.BlockSpec(memory_space=pl.ANY),
            scratch_shapes=[dma((4, J))],
            compiler_params=pltpu.CompilerParams(vmem_limit_bytes=1024 * 1024),
            name="store",
        )(pltpu.with_memory_space_constraint(held, pltpu.VMEM))

    spec = P("py", "px", None)
    return jax.shard_map(local, mesh=mesh, in_specs=(spec, spec, spec), out_specs=spec, check_vma=False)
```

```python
import jax
import jax.numpy as jnp
from jax import lax
from jax.experimental import pallas as pl
from jax.experimental.pallas import tpu as pltpu
from jax.sharding import PartitionSpec as P

MESH = pl.DeviceIdType.MESH
RATIO = 4
INNER = 13
DEPTH = 6
AGAIN = 7
PX = 8
CPX = 16


CORNERS = [(-1, -1), (-1, 1), (1, -1), (1, 1)]


def corner_cells(depth, rows, cols, dy, dx):
    cells, place = [], 0
    for k in range(1, depth):
        n = depth - k
        here, there = (k - 1, rows + k - 1) if dy < 0 else (rows - k, -k)
        cells.append((here, there, 0, cols, n, place) if dx < 0 else (here, there, cols - n, -n, n, place))
        place += n
    return cells


def kernel(ny, nx, source, initial, absorb, D,
           U, V, S, W, CL, CW, CA, CB, CC, E, T, LY, LX, KX, KC, LC,
           ld_sem, ys, yr, xs, xr, cs, cr):
    J, Y, X = S.shape[0], S.shape[1], S.shape[2]
    CY, CX = Y // RATIO, X // RATIO
    my, mx = lax.axis_index("py"), lax.axis_index("px")

    def device(dy, dx):
        return (lax.rem(my + dy + ny, ny), lax.rem(mx + dx + nx, nx))

    def loads(array, ref, padded, spans, base):
        made = []
        for low, count in spans:
            for j in range(J):
                if padded:
                    dst = ref.at[j, pl.ds(1 + low, count), pl.ds(PX, X), :]
                else:
                    dst = ref.at[j, pl.ds(low, count), :, :]
                made.append(pltpu.make_async_copy(
                    array.at[pl.ds(low, count), :, pl.ds(j * 128, 128)], dst, ld_sem.at[base + len(made)]))
        return made

    quarters = [(n * Y // 4, Y // 4) for n in range(4)]
    load_ends = loads(initial, U, True, [(0, 1), (Y - 1, 1)], 0)
    load_u = loads(initial, U, True, [(1, 15), (16, 16), (32, 16), (48, Y - 49)], 2 * J)
    load_d = loads(absorb, D, False, quarters, 6 * J)
    load_s = loads(source, S, False, quarters, 10 * J)
    for copy in load_ends + load_u + load_d + load_s:
        copy.start()

    around = [(dy, dx) for dy in (-1, 0, 1) for dx in (-1, 0, 1) if (dy, dx) != (0, 0)]
    barrier = pltpu.get_barrier_semaphore()
    for dy, dx in around:
        pl.semaphore_signal(barrier, inc=1, device_id=device(dy, dx), device_id_type=MESH)
    with jax.named_scope("barrier"):
        pl.semaphore_wait(barrier, len(around))

    def rows_copies(k, ref):
        return [
            pltpu.make_async_remote_copy(
                src_ref=ref.at[:, 1, pl.ds(PX, X), :], dst_ref=LY.at[k, 1], send_sem=ys.at[k, 1], recv_sem=yr.at[k, 1],
                device_id=device(-1, 0), device_id_type=MESH),
            pltpu.make_async_remote_copy(
                src_ref=ref.at[:, Y, pl.ds(PX, X), :], dst_ref=LY.at[k, 0], send_sem=ys.at[k, 0], recv_sem=yr.at[k, 0],
                device_id=device(1, 0), device_id_type=MESH),
        ]

    def columns_copies(k):
        return [
            pltpu.make_async_remote_copy(
                src_ref=KX.at[k, 1], dst_ref=LX.at[k, 1], send_sem=xs.at[k, 1], recv_sem=xr.at[k, 1],
                device_id=device(0, -1), device_id_type=MESH),
            pltpu.make_async_remote_copy(
                src_ref=KX.at[k, 0], dst_ref=LX.at[k, 0], send_sem=xs.at[k, 0], recv_sem=xr.at[k, 0],
                device_id=device(0, 1), device_id_type=MESH),
        ]

    def start(copies):
        for copy in copies:
            copy.start()

    def received(copies):
        for copy in copies:
            copy.wait_recv()

    def sent(copies):
        for copy in copies:
            copy.wait_send()

    def pack(k, ref):
        def body(y, carry):
            for j in range(J):
                KX[k, 1, j, pl.ds(y, 1), :] = ref[j, y + 1, pl.ds(PX, 1), :]
                KX[k, 0, j, pl.ds(y, 1), :] = ref[j, y + 1, pl.ds(PX + X - 1, 1), :]
            return carry
        lax.fori_loop(0, Y, body, 0)

    def unpack_columns(k, ref):
        def body(y, carry):
            for j in range(J):
                ref[j, y + 1, pl.ds(PX + X, 1), :] = LX[k, 1, j, pl.ds(y, 1), :]
                ref[j, y + 1, pl.ds(PX - 1, 1), :] = LX[k, 0, j, pl.ds(y, 1), :]
            return carry
        lax.fori_loop(0, Y, body, 0)

    def unpack_rows(k, ref):
        for j in range(J):
            ref[j, 0, pl.ds(PX, X), :] = LY[k, 0, j]
            ref[j, Y + 1, pl.ds(PX, X), :] = LY[k, 1, j]

    def residual_rows(src, j, y, n, x, w):
        r = [src[j, y + k, pl.ds(PX + x, w), :] for k in range(n + 2)]
        for k in range(n):
            beside = src[j, y + k + 1, pl.ds(PX + x - 1, w), :] + src[j, y + k + 1, pl.ds(PX + x + 1, w), :]
            yield k, r[k + 1], S[j, y + k, pl.ds(x, w), :] + (r[k] + r[k + 2] + beside)

    def relax(src, put, y, n, columns):
        for j in range(J):
            for x, w in columns:
                for k, old, total in residual_rows(src, j, y, n, x, w):
                    put(j, y + k, x, w, 0.2 * old + W[j, y + k, pl.ds(x, w), :] * total)

    def into(ref):
        def put(j, y, x, w, value):
            ref[j, y + 1, pl.ds(PX + x, w), :] = value
        return put

    def into_result(j, y, x, w, value):
        D[j, y, pl.ds(x, w), :] = value

    middle_columns = [(x, min(32, X - 8 - x)) for x in range(8, X - 8, 32)]
    edge_columns = [(0, 8), (X - 8, 8)]
    all_columns = [(x, 32) for x in range(0, X, 32)]

    def inner(src, put, columns):
        def body(i, carry):
            relax(src, put, 2 + 4 * i, 4, columns)
            return carry
        lax.fori_loop(0, (Y - 4) // 4, body, 0)

    def outer(src, put):
        def body(i, carry):
            relax(src, put, i * (Y - 2), 2, all_columns)
            return carry
        lax.fori_loop(0, 2, body, 0)

    def coarse_copies(ref, pieces, base):
        made = []
        for n, (dy, dx, r, nr, c, nc) in enumerate(pieces):
            made.append(pltpu.make_async_remote_copy(
                src_ref=ref.at[:, pl.ds(AGAIN + r, nr), pl.ds(CPX + c, nc), :],
                dst_ref=ref.at[:, pl.ds(AGAIN + r - CY * dy, nr), pl.ds(CPX + c - CX * dx, nc), :],
                send_sem=cs.at[base + n], recv_sem=cr.at[base + n],
                device_id=device(dy, dx), device_id_type=MESH))
        return made

    def corner_copies(which, cells, base):
        return [pltpu.make_async_remote_copy(
            src_ref=KC.at[which, n, :, pl.ds(0, cells), :], dst_ref=LC.at[which, n, :, pl.ds(0, cells), :],
            send_sem=cs.at[base + n], recv_sem=cr.at[base + n],
            device_id=device(dy, dx), device_id_type=MESH) for n, (dy, dx) in enumerate(CORNERS)]

    def pack_corners(which, ref, depth):
        for n, (dy, dx) in enumerate(CORNERS):
            for here, _, c, _, count, place in corner_cells(depth, CY, CX, dy, dx):
                for j in range(J):
                    KC[which, n, j, pl.ds(place, count), :] = ref[j, AGAIN + here, pl.ds(CPX + c, count), :]

    def unpack_corners(which, ref, depth):
        for n, (dy, dx) in enumerate(CORNERS):
            for _, there, _, c, count, place in corner_cells(depth, CY, CX, dy, dx):
                for j in range(J):
                    ref[j, AGAIN + there, pl.ds(CPX + c, count), :] = LC[which, n, j, pl.ds(place, count), :]

    def sides(first, last):
        return [(0, -1, first, last - first, 0, 8), (0, 1, first, last - first, CX - 8, 8)]

    half = DEPTH // 2
    mass_near = coarse_copies(CW, [(-1, 0, 0, half, 0, CX), (1, 0, CY - half, half, 0, CX)], 0)
    mass_far = coarse_copies(
        CW, [(-1, 0, half, DEPTH - half, 0, CX), (1, 0, CY - DEPTH, DEPTH - half, 0, CX)] + sides(0, CY), 2)
    mass_corners = corner_copies(0, 16, 6)
    load_early = coarse_copies(CL, [(-1, 0, 1, DEPTH - 1, 0, CX), (1, 0, CY - DEPTH, DEPTH - 1, 0, CX)], 10)
    load_late = coarse_copies(CL, [(-1, 0, 0, 1, 0, CX), (1, 0, CY - 1, 1, 0, CX)] + sides(0, CY), 12)
    load_corners = corner_copies(1, 16, 16)
    value_copies = coarse_copies(CC, [(-1, 0, 0, AGAIN, 0, CX), (1, 0, CY - AGAIN, AGAIN, 0, CX)] + sides(0, CY), 20)
    value_corners = corner_copies(2, 24, 24)

    rows0, rows1, rows2, rows3 = (rows_copies(0, U), rows_copies(1, V), rows_copies(2, U), rows_copies(3, V))
    cols0, cols1, cols2, cols3 = (columns_copies(0), columns_copies(1), columns_copies(2), columns_copies(3))
    with jax.named_scope("wait_ends"):
        for copy in load_ends:
            copy.wait()
        start(rows0)
    with jax.named_scope("wait_u"):
        for copy in load_u:
            copy.wait()
    with jax.named_scope("pack0"):
        pack(0, U)
        start(cols0)

    with jax.named_scope("wait_d"):
        for copy in load_d:
            copy.wait()

    def fold(ref, j):
        return (ref[j, pl.ds(0, CX, stride=RATIO), :] + ref[j, pl.ds(1, CX, stride=RATIO), :]
                + ref[j, pl.ds(2, CX, stride=RATIO), :] + ref[j, pl.ds(3, CX, stride=RATIO), :])

    def weight_row(cy, carry):
        for j in range(J):
            total = jnp.zeros((X, 128), jnp.float32)
            for r in range(RATIO):
                mass = D[j, cy * RATIO + r]
                total = total + mass
                whole = 4.0 + mass
                D[j, cy * RATIO + r] = whole
                W[j, cy * RATIO + r] = 0.8 / whole
            T[j, 0] = total
            CW[j, AGAIN + cy, pl.ds(CPX, CX), :] = 0.8 / (4.0 + 0.25 * fold(T.at[:, 0], j))
        return carry
    with jax.named_scope("weights"):
        lax.fori_loop(0, CY, weight_row, 0)
        start(mass_near)

    with jax.named_scope("wait_s"):
        for copy in load_s:
            copy.wait()
    with jax.named_scope("middle1"):
        inner(U, into(V), middle_columns)
    with jax.named_scope("wait_x0"):
        received(cols0)
    with jax.named_scope("edges1"):
        unpack_columns(0, U)
        inner(U, into(V), edge_columns)
    with jax.named_scope("wait_y0"):
        received(rows0)
    with jax.named_scope("outer1"):
        unpack_rows(0, U)
        outer(U, into(V))
        start(rows1)
        pack(1, V)
        start(cols1)
        start(mass_far)
        pack_corners(0, CW, DEPTH)
        start(mass_corners)

    sent(rows0)
    with jax.named_scope("middle2"):
        inner(V, into(U), middle_columns)
    with jax.named_scope("wait_x1"):
        received(cols1)
    with jax.named_scope("edges2"):
        unpack_columns(1, V)
        inner(V, into(U), edge_columns)
    with jax.named_scope("wait_y1"):
        received(rows1)
    with jax.named_scope("outer2"):
        unpack_rows(1, V)
        outer(V, into(U))
        start(rows2)
        pack(2, U)
        start(cols2)

    def defect(cy, columns):
        for j in range(J):
            for x, w in columns:
                total = None
                for k, old, around in residual_rows(U, j, cy * RATIO, RATIO, x, w):
                    term = around - D[j, cy * RATIO + k, pl.ds(x, w), :] * old
                    total = term if total is None else total + term
                T[j, cy, pl.ds(x, w), :] = total

    def coarse_load(cy):
        for j in range(J):
            CL[j, AGAIN + cy, pl.ds(CPX, CX), :] = 0.25 * fold(T.at[:, cy], j)

    def defect_middle(cy, carry):
        defect(cy, middle_columns)
        return carry

    def defect_edges(cy, carry):
        defect(cy, edge_columns)
        coarse_load(cy)
        return carry

    def defect_ends(i, carry):
        defect(i * (CY - 1), all_columns)
        coarse_load(i * (CY - 1))
        return carry

    with jax.named_scope("defect_middle"):
        lax.fori_loop(1, CY - 1, defect_middle, 0)
    with jax.named_scope("wait_x2"):
        received(cols2)
    with jax.named_scope("defect_edges"):
        unpack_columns(2, U)
        lax.fori_loop(1, CY - 1, defect_edges, 0)
        start(load_early)
    with jax.named_scope("wait_y2"):
        received(rows2)
    with jax.named_scope("defect_ends"):
        unpack_rows(2, U)
        lax.fori_loop(0, 2, defect_ends, 0)
        start(load_late)
        pack_corners(1, CL, DEPTH)
        start(load_corners)
    with jax.named_scope("wait_mass"):
        received(mass_near + mass_far + mass_corners)
        unpack_corners(0, CW, DEPTH)
    with jax.named_scope("wait_load"):
        received(load_early + load_late + load_corners)
        unpack_corners(1, CL, DEPTH)

    def first(y, carry):
        for j in range(J):
            CA[j, y] = CW[j, y] * CL[j, y]
        return carry

    def coarse_sweep(old, new, reach):
        x0 = CPX - 8 if reach > 0 else CPX
        wide = CX + 2 * (CPX - x0)

        n = 4 if (CY + 2 * reach) % 4 == 0 else 2
        half = wide // 2

        def coarse_rows(i, carry):
            y = AGAIN - reach + n * i
            for j in range(J):
                for x in (x0, x0 + half):
                    r = [old[j, y - 1 + k, pl.ds(x, half), :] for k in range(n + 2)]
                    for k in range(n):
                        beside = old[j, y + k, pl.ds(x - 1, half), :] + old[j, y + k, pl.ds(x + 1, half), :]
                        total = CL[j, y + k, pl.ds(x, half), :] + (r[k] + r[k + 2] + beside)
                        new[j, y + k, pl.ds(x, half), :] = 0.2 * r[k + 1] + CW[j, y + k, pl.ds(x, half), :] * total
            return carry
        lax.fori_loop(0, (CY + 2 * reach) // n, coarse_rows, 0)

    with jax.named_scope("coarse1"):
        lax.fori_loop(AGAIN - DEPTH, AGAIN + CY + DEPTH, first, 0)
        old, new = CA, CB
        for reach in range(DEPTH - 1, -1, -1):
            coarse_sweep(old, CC if reach == 0 else new, reach)
            old, new = new, old
        start(value_copies)
        pack_corners(2, CC, AGAIN)
        start(value_corners)
    with jax.named_scope("wait_value"):
        received(value_copies + value_corners)
        unpack_corners(2, CC, AGAIN)
    with jax.named_scope("coarse2"):
        old, new = CC, CA
        for reach in range(AGAIN - 1, 0, -1):
            coarse_sweep(old, new, reach)
            old, new = new, (CB if new is CA else CA)
        C = old

    def spread(cy):
        for j in range(J):
            cells = C[j, AGAIN + cy, pl.ds(CPX, CX), :]
            for k in range(RATIO):
                E[j, pl.ds(PX + k, CX, stride=RATIO), :] = cells
            E[j, pl.ds(PX - 1, 1), :] = C[j, AGAIN + cy, pl.ds(CPX - 1, 1), :]
            E[j, pl.ds(PX + X, 1), :] = C[j, AGAIN + cy, pl.ds(CPX + CX, 1), :]

    def add_row(y):
        for j in range(J):
            U[j, y] = U[j, y] + E[j]

    sent(rows2)

    def correct(cy, carry):
        spread(cy)
        for r in range(RATIO):
            add_row(1 + cy * RATIO + r)
        return carry

    spread(-1)
    add_row(0)
    with jax.named_scope("correct"):
        lax.fori_loop(0, CY, correct, 0)
        spread(CY)
        add_row(Y + 1)

    sent(rows1)
    with jax.named_scope("outer3"):
        outer(U, into(V))
        start(rows3)
    with jax.named_scope("sweep3"):
        inner(U, into(V), edge_columns)
        pack(3, V)
        start(cols3)
        inner(U, into(V), middle_columns)
    with jax.named_scope("middle4"):
        inner(V, into_result, middle_columns)
    with jax.named_scope("wait_x3"):
        received(cols3)
    with jax.named_scope("edges4"):
        unpack_columns(3, V)
        inner(V, into_result, edge_columns)
    with jax.named_scope("wait_y3"):
        received(rows3)
    with jax.named_scope("outer4"):
        unpack_rows(3, V)
        outer(V, into_result)
    sent(rows3)
    for copies in (cols0, cols1, cols2, cols3, mass_near, mass_far, mass_corners, load_early, load_late, load_corners,
                   value_copies, value_corners):
        sent(copies)


def store(held, out, sems):
    J, Y, X = held.shape[0], held.shape[1], held.shape[2]
    copies = []
    for n in range(4):
        for j in range(J):
            rows = pl.ds(n * Y // 4, Y // 4)
            copies.append(pltpu.make_async_copy(held.at[j, rows], out.at[rows, :, pl.ds(j * 128, 128)], sems.at[n, j]))
    for copy in copies:
        copy.start()
    for copy in copies:
        copy.wait()


def solution(mesh):
    ny, nx = mesh.shape["py"], mesh.shape["px"]

    def local(source_terms, initial_values, absorption):
        Y, X, cases = source_terms.shape
        J = cases // 128
        CY, CX = Y // RATIO, X // RATIO
        f32 = jnp.float32
        fine = pltpu.VMEM((J, Y + 2, X + 2 * PX, 128), f32)
        plain = pltpu.VMEM((J, Y, X, 128), f32)
        coarse = pltpu.VMEM((J, CY + 2 * AGAIN, CX + 2 * CPX, 128), f32)
        dma = pltpu.SemaphoreType.DMA

        def body(*refs):
            kernel(ny, nx, *refs)

        held = pl.pallas_call(
            body,
            out_shape=plain,
            in_specs=[pl.BlockSpec(memory_space=pl.ANY)] * 3,
            out_specs=pl.BlockSpec(memory_space=pltpu.VMEM),
            scratch_shapes=[
                fine, fine, plain, plain, coarse, coarse, coarse, coarse, coarse,
                pltpu.VMEM((J, X + 2 * PX, 128), f32),
                pltpu.VMEM((J, CY, X, 128), f32),
                pltpu.VMEM((4, 2, J, X, 128), f32),
                pltpu.VMEM((4, 2, J, Y, 128), f32),
                pltpu.VMEM((4, 2, J, Y, 128), f32),
                pltpu.VMEM((3, 4, J, 24, 128), f32),
                pltpu.VMEM((3, 4, J, 24, 128), f32),
                dma((14 * J,)),
                dma((4, 2)), dma((4, 2)), dma((4, 2)), dma((4, 2)),
                dma((28,)), dma((28,)),
            ],
            compiler_params=pltpu.CompilerParams(
                collective_id=0, has_side_effects=True, vmem_limit_bytes=52 * 1024 * 1024),
            name="two_grid",
        )(source_terms, initial_values, absorption)
        return pl.pallas_call(
            store,
            out_shape=jax.ShapeDtypeStruct((Y, X, cases), f32),
            in_specs=[pl.BlockSpec(memory_space=pltpu.VMEM)],
            out_specs=pl.BlockSpec(memory_space=pl.ANY),
            scratch_shapes=[dma((4, J))],
            compiler_params=pltpu.CompilerParams(vmem_limit_bytes=1024 * 1024),
            name="store",
        )(pltpu.with_memory_space_constraint(held, pltpu.VMEM))

    spec = P("py", "px", None)
    return jax.shard_map(local, mesh=mesh, in_specs=(spec, spec, spec), out_specs=spec, check_vma=False)
```

```python
import jax
import jax.numpy as jnp
from jax import lax
from jax.experimental import pallas as pl
from jax.experimental.pallas import tpu as pltpu
from jax.sharding import PartitionSpec as P

MESH = pl.DeviceIdType.MESH
RATIO = 4
INNER = 13
DEPTH = 6
AGAIN = 7
PX = 8
CPX = 16


CORNERS = [(-1, -1), (-1, 1), (1, -1), (1, 1)]


def corner_cells(depth, rows, cols, dy, dx):
    cells, place = [], 0
    for k in range(1, depth):
        n = depth - k
        here, there = (k - 1, rows + k - 1) if dy < 0 else (rows - k, -k)
        cells.append((here, there, 0, cols, n, place) if dx < 0 else (here, there, cols - n, -n, n, place))
        place += n
    return cells


def kernel(ny, nx, source, initial, absorb, D,
           U, V, S, W, CL, CW, CA, CB, CC, E, T, LY, LX, KX, KC, LC,
           ld_sem, ys, yr, xs, xr, cs, cr):
    J, Y, X = S.shape[0], S.shape[1], S.shape[2]
    CY, CX = Y // RATIO, X // RATIO
    my, mx = lax.axis_index("py"), lax.axis_index("px")

    def device(dy, dx):
        return (lax.rem(my + dy + ny, ny), lax.rem(mx + dx + nx, nx))

    def loads(array, ref, padded, spans, base, x=0, w=X):
        made = []
        for low, count in spans:
            for j in range(J):
                if padded:
                    dst = ref.at[j, pl.ds(1 + low, count), pl.ds(PX + x, w), :]
                else:
                    dst = ref.at[j, pl.ds(low, count), :, :]
                made.append(pltpu.make_async_copy(
                    array.at[pl.ds(low, count), pl.ds(x, w), pl.ds(j * 128, 128)], dst, ld_sem.at[base + len(made)]))
        return made

    quarters = [(n * Y // 4, Y // 4) for n in range(4)]
    load_ends = loads(initial, U, True, [(0, 1), (Y - 1, 1)], 0, 8, X - 16)
    load_tiles = [pltpu.make_async_copy(
        initial.at[:, pl.ds(x, 8), pl.ds(j * 128, 128)], U.at[j, pl.ds(1, Y), pl.ds(PX + x, 8), :],
        ld_sem.at[16 * J + 2 * j + n]) for j in range(J) for n, x in enumerate((0, X - 8))]
    load_u = loads(initial, U, True, [(1, 15), (16, 16), (32, 16), (48, Y - 49)], 2 * J, 8, X - 16)
    load_d = [pltpu.make_async_copy(absorb.at[pl.ds(low, count)], D.at[pl.ds(low, count)], ld_sem.at[6 * J + n])
              for n, (low, count) in enumerate(quarters)]
    load_near = loads(source, S, False, [(0, 4), (Y - 4, 4)], 10 * J)
    load_s = loads(source, S, False, [(4, 12), (16, 16), (32, 16), (48, Y - 52)], 12 * J)
    for copy in load_ends + load_tiles + load_u + load_near + load_d + load_s:
        copy.start()

    around = [(dy, dx) for dy in (-1, 0, 1) for dx in (-1, 0, 1) if (dy, dx) != (0, 0)]
    barrier = pltpu.get_barrier_semaphore()
    for dy, dx in around:
        pl.semaphore_signal(barrier, inc=1, device_id=device(dy, dx), device_id_type=MESH)
    with jax.named_scope("barrier"):
        pl.semaphore_wait(barrier, len(around))

    def rows_copies(k, ref):
        return [
            pltpu.make_async_remote_copy(
                src_ref=ref.at[:, 1, pl.ds(PX, X), :], dst_ref=LY.at[k, 1], send_sem=ys.at[k, 1], recv_sem=yr.at[k, 1],
                device_id=device(-1, 0), device_id_type=MESH),
            pltpu.make_async_remote_copy(
                src_ref=ref.at[:, Y, pl.ds(PX, X), :], dst_ref=LY.at[k, 0], send_sem=ys.at[k, 0], recv_sem=yr.at[k, 0],
                device_id=device(1, 0), device_id_type=MESH),
        ]

    def columns_copies(k):
        return [
            pltpu.make_async_remote_copy(
                src_ref=KX.at[k, 1], dst_ref=LX.at[k, 1], send_sem=xs.at[k, 1], recv_sem=xr.at[k, 1],
                device_id=device(0, -1), device_id_type=MESH),
            pltpu.make_async_remote_copy(
                src_ref=KX.at[k, 0], dst_ref=LX.at[k, 0], send_sem=xs.at[k, 0], recv_sem=xr.at[k, 0],
                device_id=device(0, 1), device_id_type=MESH),
        ]

    def start(copies):
        for copy in copies:
            copy.start()

    def received(copies):
        for copy in copies:
            copy.wait_recv()

    def sent(copies):
        for copy in copies:
            copy.wait_send()

    def pack(k, ref):
        def body(y, carry):
            for j in range(J):
                KX[k, 1, j, pl.ds(y, 1), :] = ref[j, y + 1, pl.ds(PX, 1), :]
                KX[k, 0, j, pl.ds(y, 1), :] = ref[j, y + 1, pl.ds(PX + X - 1, 1), :]
            return carry
        lax.fori_loop(0, Y, body, 0)

    def unpack_columns(k, ref):
        def body(y, carry):
            for j in range(J):
                ref[j, y + 1, pl.ds(PX + X, 1), :] = LX[k, 1, j, pl.ds(y, 1), :]
                ref[j, y + 1, pl.ds(PX - 1, 1), :] = LX[k, 0, j, pl.ds(y, 1), :]
            return carry
        lax.fori_loop(0, Y, body, 0)

    def unpack_rows(k, ref):
        for j in range(J):
            ref[j, 0, pl.ds(PX, X), :] = LY[k, 0, j]
            ref[j, Y + 1, pl.ds(PX, X), :] = LY[k, 1, j]

    def residual_rows(src, j, y, n, x, w):
        r = [src[j, y + k, pl.ds(PX + x, w), :] for k in range(n + 2)]
        for k in range(n):
            beside = src[j, y + k + 1, pl.ds(PX + x - 1, w), :] + src[j, y + k + 1, pl.ds(PX + x + 1, w), :]
            yield k, r[k + 1], S[j, y + k, pl.ds(x, w), :] + (r[k] + r[k + 2] + beside)

    def relax(src, put, y, n, columns):
        for j in range(J):
            for x, w in columns:
                for k, old, total in residual_rows(src, j, y, n, x, w):
                    put(j, y + k, x, w, 0.2 * old + W[j, y + k, pl.ds(x, w), :] * total)

    def into(ref):
        def put(j, y, x, w, value):
            ref[j, y + 1, pl.ds(PX + x, w), :] = value
        return put

    def into_result(j, y, x, w, value):
        D[y, pl.ds(x, w), pl.ds(j * 128, 128)] = value

    middle_columns = [(x, min(32, X - 8 - x)) for x in range(8, X - 8, 32)]
    edge_columns = [(0, 8), (X - 8, 8)]
    all_columns = [(x, 32) for x in range(0, X, 32)]

    def inner(src, put, columns):
        def body(i, carry):
            relax(src, put, 2 + 4 * i, 4, columns)
            return carry
        lax.fori_loop(0, (Y - 4) // 4, body, 0)

    def outer(src, put):
        def body(i, carry):
            relax(src, put, i * (Y - 2), 2, all_columns)
            return carry
        lax.fori_loop(0, 2, body, 0)

    def coarse_copies(ref, pieces, base):
        made = []
        for n, (dy, dx, r, nr, c, nc) in enumerate(pieces):
            made.append(pltpu.make_async_remote_copy(
                src_ref=ref.at[:, pl.ds(AGAIN + r, nr), pl.ds(CPX + c, nc), :],
                dst_ref=ref.at[:, pl.ds(AGAIN + r - CY * dy, nr), pl.ds(CPX + c - CX * dx, nc), :],
                send_sem=cs.at[base + n], recv_sem=cr.at[base + n],
                device_id=device(dy, dx), device_id_type=MESH))
        return made

    def corner_copies(which, cells, base):
        return [pltpu.make_async_remote_copy(
            src_ref=KC.at[which, n, :, pl.ds(0, cells), :], dst_ref=LC.at[which, n, :, pl.ds(0, cells), :],
            send_sem=cs.at[base + n], recv_sem=cr.at[base + n],
            device_id=device(dy, dx), device_id_type=MESH) for n, (dy, dx) in enumerate(CORNERS)]

    def pack_corners(which, ref, depth):
        for n, (dy, dx) in enumerate(CORNERS):
            for here, _, c, _, count, place in corner_cells(depth, CY, CX, dy, dx):
                for j in range(J):
                    KC[which, n, j, pl.ds(place, count), :] = ref[j, AGAIN + here, pl.ds(CPX + c, count), :]

    def unpack_corners(which, ref, depth):
        for n, (dy, dx) in enumerate(CORNERS):
            for _, there, _, c, count, place in corner_cells(depth, CY, CX, dy, dx):
                for j in range(J):
                    ref[j, AGAIN + there, pl.ds(CPX + c, count), :] = LC[which, n, j, pl.ds(place, count), :]

    def sides(first, last):
        return [(0, -1, first, last - first, 0, 8), (0, 1, first, last - first, CX - 8, 8)]

    half = DEPTH // 2
    mass_near = coarse_copies(CW, [(-1, 0, 0, half, 0, CX), (1, 0, CY - half, half, 0, CX)], 0)
    mass_far = coarse_copies(
        CW, [(-1, 0, half, DEPTH - half, 0, CX), (1, 0, CY - DEPTH, DEPTH - half, 0, CX)] + sides(0, CY), 2)
    mass_corners = corner_copies(0, 16, 6)
    load_early = coarse_copies(CL, [(-1, 0, 1, DEPTH - 1, 0, CX), (1, 0, CY - DEPTH, DEPTH - 1, 0, CX)], 10)
    load_late = coarse_copies(CL, [(-1, 0, 0, 1, 0, CX), (1, 0, CY - 1, 1, 0, CX)] + sides(0, CY), 12)
    load_corners = corner_copies(1, 16, 16)
    value_copies = coarse_copies(CC, [(-1, 0, 0, AGAIN, 0, CX), (1, 0, CY - AGAIN, AGAIN, 0, CX)] + sides(0, CY), 20)
    value_corners = corner_copies(2, 24, 24)

    rows0, rows1, rows2, rows3 = (rows_copies(0, U), rows_copies(1, V), rows_copies(2, U), rows_copies(3, V))
    cols0, cols1, cols2, cols3 = (columns_copies(0), columns_copies(1), columns_copies(2), columns_copies(3))
    with jax.named_scope("wait_ends"):
        for copy in load_ends + load_tiles:
            copy.wait()
        start(rows0)
    with jax.named_scope("pack0"):
        pack(0, U)
        start(cols0)
    with jax.named_scope("wait_u"):
        for copy in load_u:
            copy.wait()

    with jax.named_scope("wait_d"):
        for copy in load_d:
            copy.wait()

    def fold(ref, j):
        return (ref[j, pl.ds(0, CX, stride=RATIO), :] + ref[j, pl.ds(1, CX, stride=RATIO), :]
                + ref[j, pl.ds(2, CX, stride=RATIO), :] + ref[j, pl.ds(3, CX, stride=RATIO), :])

    def weight_row(cy, carry):
        for j in range(J):
            total = jnp.zeros((X, 128), jnp.float32)
            for r in range(RATIO):
                mass = D[cy * RATIO + r, :, pl.ds(j * 128, 128)]
                total = total + mass
                whole = 4.0 + mass
                D[cy * RATIO + r, :, pl.ds(j * 128, 128)] = whole
                W[j, cy * RATIO + r] = 0.8 / whole
            T[j, 0] = total
            CW[j, AGAIN + cy, pl.ds(CPX, CX), :] = 0.8 / (4.0 + 0.25 * fold(T.at[:, 0], j))
        return carry
    with jax.named_scope("weights"):
        lax.fori_loop(0, CY, weight_row, 0)
        start(mass_near)

    with jax.named_scope("wait_x0"):
        for copy in load_near:
            copy.wait()
        received(cols0)
    with jax.named_scope("unpack0"):
        unpack_columns(0, U)
    with jax.named_scope("wait_y0"):
        received(rows0)
    with jax.named_scope("outer1"):
        unpack_rows(0, U)
        outer(U, into(V))
        start(rows1)
    with jax.named_scope("wait_s"):
        for copy in load_s:
            copy.wait()
    with jax.named_scope("edges1"):
        inner(U, into(V), edge_columns)
        pack(1, V)
        start(cols1)
        start(mass_far)
        pack_corners(0, CW, DEPTH)
        start(mass_corners)
    with jax.named_scope("middle1"):
        inner(U, into(V), middle_columns)

    sent(rows0)
    with jax.named_scope("middle2"):
        inner(V, into(U), middle_columns)
    with jax.named_scope("wait_x1"):
        received(cols1)
    with jax.named_scope("edges2"):
        unpack_columns(1, V)
        inner(V, into(U), edge_columns)
    with jax.named_scope("wait_y1"):
        received(rows1)
    with jax.named_scope("outer2"):
        unpack_rows(1, V)
        outer(V, into(U))
        start(rows2)
        pack(2, U)
        start(cols2)

    def defect(cy, columns):
        for j in range(J):
            for x, w in columns:
                total = None
                for k, old, around in residual_rows(U, j, cy * RATIO, RATIO, x, w):
                    term = around - D[cy * RATIO + k, pl.ds(x, w), pl.ds(j * 128, 128)] * old
                    total = term if total is None else total + term
                T[j, cy, pl.ds(x, w), :] = total

    def coarse_load(cy):
        for j in range(J):
            CL[j, AGAIN + cy, pl.ds(CPX, CX), :] = 0.25 * fold(T.at[:, cy], j)

    def defect_middle(cy, carry):
        defect(cy, middle_columns)
        return carry

    def defect_edges(cy, carry):
        defect(cy, edge_columns)
        coarse_load(cy)
        return carry

    def defect_ends(i, carry):
        defect(i * (CY - 1), all_columns)
        coarse_load(i * (CY - 1))
        return carry

    with jax.named_scope("defect_middle"):
        lax.fori_loop(1, CY - 1, defect_middle, 0)
    with jax.named_scope("wait_x2"):
        received(cols2)
    with jax.named_scope("defect_edges"):
        unpack_columns(2, U)
        lax.fori_loop(1, CY - 1, defect_edges, 0)
        start(load_early)
    with jax.named_scope("wait_y2"):
        received(rows2)
    with jax.named_scope("defect_ends"):
        unpack_rows(2, U)
        lax.fori_loop(0, 2, defect_ends, 0)
        start(load_late)
        pack_corners(1, CL, DEPTH)
        start(load_corners)
    with jax.named_scope("wait_mass"):
        received(mass_near + mass_far + mass_corners)
        unpack_corners(0, CW, DEPTH)
    with jax.named_scope("wait_load"):
        received(load_early + load_late + load_corners)
        unpack_corners(1, CL, DEPTH)

    def first(y, carry):
        for j in range(J):
            CA[j, y, pl.ds(CPX - 8, CX + 16), :] = CW[j, y, pl.ds(CPX - 8, CX + 16), :] * CL[j, y, pl.ds(CPX - 8, CX + 16), :]
        return carry

    def coarse_sweep(old, new, reach):
        x0 = CPX - 8 if reach > 0 else CPX
        wide = CX + 2 * (CPX - x0)

        n = 4 if (CY + 2 * reach) % 4 == 0 else 2
        half = wide // 2

        def coarse_rows(i, carry):
            y = AGAIN - reach + n * i
            for j in range(J):
                for x in (x0, x0 + half):
                    r = [old[j, y - 1 + k, pl.ds(x, half), :] for k in range(n + 2)]
                    for k in range(n):
                        beside = old[j, y + k, pl.ds(x - 1, half), :] + old[j, y + k, pl.ds(x + 1, half), :]
                        total = CL[j, y + k, pl.ds(x, half), :] + (r[k] + r[k + 2] + beside)
                        new[j, y + k, pl.ds(x, half), :] = 0.2 * r[k + 1] + CW[j, y + k, pl.ds(x, half), :] * total
            return carry
        lax.fori_loop(0, (CY + 2 * reach) // n, coarse_rows, 0)

    with jax.named_scope("coarse1"):
        lax.fori_loop(AGAIN - DEPTH, AGAIN + CY + DEPTH, first, 0)
        old, new = CA, CB
        for reach in range(DEPTH - 1, -1, -1):
            coarse_sweep(old, CC if reach == 0 else new, reach)
            old, new = new, old
        start(value_copies)
        pack_corners(2, CC, AGAIN)
        start(value_corners)
    with jax.named_scope("wait_value"):
        received(value_copies + value_corners)
        unpack_corners(2, CC, AGAIN)
    with jax.named_scope("coarse2"):
        old, new = CC, CA
        for reach in range(AGAIN - 1, 0, -1):
            coarse_sweep(old, new, reach)
            old, new = new, (CB if new is CA else CA)
        C = old

    def spread(cy):
        for j in range(J):
            cells = C[j, AGAIN + cy, pl.ds(CPX, CX), :]
            for k in range(RATIO):
                E[j, pl.ds(PX + k, CX, stride=RATIO), :] = cells
            E[j, pl.ds(PX - 1, 1), :] = C[j, AGAIN + cy, pl.ds(CPX - 1, 1), :]
            E[j, pl.ds(PX + X, 1), :] = C[j, AGAIN + cy, pl.ds(CPX + CX, 1), :]

    def add_row(y):
        for j in range(J):
            U[j, y] = U[j, y] + E[j]

    sent(rows2)

    def correct(cy, carry):
        spread(cy)
        for r in range(RATIO):
            add_row(1 + cy * RATIO + r)
        return carry

    with jax.named_scope("correct_outer"):
        spread(-1)
        add_row(0)
        spread(CY)
        add_row(Y + 1)
        lax.fori_loop(0, 2, lambda i, carry: correct(i * (CY - 1), carry), 0)
    sent(rows1)
    with jax.named_scope("outer3"):
        outer(U, into(V))
        start(rows3)
    with jax.named_scope("correct"):
        lax.fori_loop(1, CY - 1, correct, 0)
    with jax.named_scope("sweep3"):
        inner(U, into(V), edge_columns)
        pack(3, V)
        start(cols3)
        inner(U, into(V), middle_columns)
    with jax.named_scope("middle4"):
        inner(V, into_result, middle_columns)
    with jax.named_scope("wait_x3"):
        received(cols3)
    with jax.named_scope("edges4"):
        unpack_columns(3, V)
        inner(V, into_result, edge_columns)
    with jax.named_scope("wait_y3"):
        received(rows3)
    with jax.named_scope("outer4"):
        unpack_rows(3, V)
        outer(V, into_result)
    sent(rows3)
    for copies in (cols0, cols1, cols2, cols3, mass_near, mass_far, mass_corners, load_early, load_late, load_corners,
                   value_copies, value_corners):
        sent(copies)


def store(held, out, sems):
    pieces = sems.shape[0]
    rows = held.shape[0] // pieces
    copies = [pltpu.make_async_copy(held.at[pl.ds(n * rows, rows)], out.at[pl.ds(n * rows, rows)], sems.at[n]) for n in range(pieces)]
    for copy in copies:
        copy.start()
    for copy in copies:
        copy.wait()


def solution(mesh):
    ny, nx = mesh.shape["py"], mesh.shape["px"]

    def local(source_terms, initial_values, absorption):
        Y, X, cases = source_terms.shape
        J = cases // 128
        CY, CX = Y // RATIO, X // RATIO
        f32 = jnp.float32
        fine = pltpu.VMEM((J, Y + 2, X + 2 * PX, 128), f32)
        plain = pltpu.VMEM((J, Y, X, 128), f32)
        coarse = pltpu.VMEM((J, CY + 2 * AGAIN, CX + 2 * CPX, 128), f32)
        dma = pltpu.SemaphoreType.DMA

        def body(*refs):
            kernel(ny, nx, *refs)

        held = pl.pallas_call(
            body,
            out_shape=pltpu.VMEM((Y, X, cases), f32),
            in_specs=[pl.BlockSpec(memory_space=pl.ANY)] * 3,
            out_specs=pl.BlockSpec(memory_space=pltpu.VMEM),
            scratch_shapes=[
                fine, fine, plain, plain, coarse, coarse, coarse, coarse, coarse,
                pltpu.VMEM((J, X + 2 * PX, 128), f32),
                pltpu.VMEM((J, CY, X, 128), f32),
                pltpu.VMEM((4, 2, J, X, 128), f32),
                pltpu.VMEM((4, 2, J, Y, 128), f32),
                pltpu.VMEM((4, 2, J, Y, 128), f32),
                pltpu.VMEM((3, 4, J, 24, 128), f32),
                pltpu.VMEM((3, 4, J, 24, 128), f32),
                dma((18 * J,)),
                dma((4, 2)), dma((4, 2)), dma((4, 2)), dma((4, 2)),
                dma((28,)), dma((28,)),
            ],
            compiler_params=pltpu.CompilerParams(
                collective_id=0, has_side_effects=True, vmem_limit_bytes=52 * 1024 * 1024),
            name="two_grid",
        )(source_terms, initial_values, absorption)
        return pl.pallas_call(
            store,
            out_shape=jax.ShapeDtypeStruct((Y, X, cases), f32),
            in_specs=[pl.BlockSpec(memory_space=pltpu.VMEM)],
            out_specs=pl.BlockSpec(memory_space=pl.ANY),
            scratch_shapes=[dma((8,))],
            compiler_params=pltpu.CompilerParams(vmem_limit_bytes=1024 * 1024),
            name="store",
        )(pltpu.with_memory_space_constraint(held, pltpu.VMEM))

    spec = P("py", "px", None)
    return jax.shard_map(local, mesh=mesh, in_specs=(spec, spec, spec), out_specs=spec, check_vma=False)
```

```python
import jax
import jax.numpy as jnp
from jax import lax
from jax.experimental import pallas as pl
from jax.experimental.pallas import tpu as pltpu
from jax.sharding import PartitionSpec as P

MESH = pl.DeviceIdType.MESH
RATIO = 4
INNER = 13
DEPTH = 6
AGAIN = 7
PX = 8
CPX = 16


CORNERS = [(-1, -1), (-1, 1), (1, -1), (1, 1)]


def corner_cells(depth, rows, cols, dy, dx):
    cells, place = [], 0
    for k in range(1, depth):
        n = depth - k
        here, there = (k - 1, rows + k - 1) if dy < 0 else (rows - k, -k)
        cells.append((here, there, 0, cols, n, place) if dx < 0 else (here, there, cols - n, -n, n, place))
        place += n
    return cells


def kernel(ny, nx, source, initial, absorb, D,
           U, V, S, W, CL, CW, CA, CB, CC, E, T, LY, LX, KX, KC, LC,
           ld_sem, ys, yr, xs, xr, cs, cr):
    J, Y, X = S.shape[0], S.shape[1], S.shape[2]
    CY, CX = Y // RATIO, X // RATIO
    my, mx = lax.axis_index("py"), lax.axis_index("px")

    def device(dy, dx):
        return (lax.rem(my + dy + ny, ny), lax.rem(mx + dx + nx, nx))

    def loads(array, ref, padded, spans, base, x=0, w=X):
        made = []
        for low, count in spans:
            for j in range(J):
                if padded:
                    dst = ref.at[j, pl.ds(1 + low, count), pl.ds(PX + x, w), :]
                else:
                    dst = ref.at[j, pl.ds(low, count), :, :]
                made.append(pltpu.make_async_copy(
                    array.at[pl.ds(low, count), pl.ds(x, w), pl.ds(j * 128, 128)], dst, ld_sem.at[base + len(made)]))
        return made

    quarters = [(n * Y // 4, Y // 4) for n in range(4)]
    load_ends = loads(initial, U, True, [(0, 1), (Y - 1, 1)], 0, 8, X - 16)
    load_tiles = [pltpu.make_async_copy(
        initial.at[:, pl.ds(x, 8), pl.ds(j * 128, 128)], U.at[j, pl.ds(1, Y), pl.ds(PX + x, 8), :],
        ld_sem.at[16 * J + 2 * j + n]) for j in range(J) for n, x in enumerate((0, X - 8))]
    load_u = loads(initial, U, True, [(1, 15), (16, 16), (32, 16), (48, Y - 49)], 2 * J, 8, X - 16)
    load_d = [pltpu.make_async_copy(absorb.at[pl.ds(low, count)], D.at[pl.ds(low, count)], ld_sem.at[6 * J + n])
              for n, (low, count) in enumerate(quarters)]
    load_near = loads(source, S, False, [(0, 4), (Y - 4, 4)], 10 * J)
    load_s = loads(source, S, False, [(4, 12), (16, 16), (32, 16), (48, Y - 52)], 12 * J)
    for copy in load_ends + load_tiles + load_u + load_near + load_d + load_s:
        copy.start()

    around = [(dy, dx) for dy in (-1, 0, 1) for dx in (-1, 0, 1) if (dy, dx) != (0, 0)]
    barrier = pltpu.get_barrier_semaphore()
    for dy, dx in around:
        pl.semaphore_signal(barrier, inc=1, device_id=device(dy, dx), device_id_type=MESH)
    with jax.named_scope("barrier"):
        pl.semaphore_wait(barrier, len(around))

    def rows_copies(k, ref):
        return [
            pltpu.make_async_remote_copy(
                src_ref=ref.at[:, 1, pl.ds(PX, X), :], dst_ref=LY.at[k, 1], send_sem=ys.at[k, 1], recv_sem=yr.at[k, 1],
                device_id=device(-1, 0), device_id_type=MESH),
            pltpu.make_async_remote_copy(
                src_ref=ref.at[:, Y, pl.ds(PX, X), :], dst_ref=LY.at[k, 0], send_sem=ys.at[k, 0], recv_sem=yr.at[k, 0],
                device_id=device(1, 0), device_id_type=MESH),
        ]

    def columns_copies(k):
        return [
            pltpu.make_async_remote_copy(
                src_ref=KX.at[k, 1], dst_ref=LX.at[k, 1], send_sem=xs.at[k, 1], recv_sem=xr.at[k, 1],
                device_id=device(0, -1), device_id_type=MESH),
            pltpu.make_async_remote_copy(
                src_ref=KX.at[k, 0], dst_ref=LX.at[k, 0], send_sem=xs.at[k, 0], recv_sem=xr.at[k, 0],
                device_id=device(0, 1), device_id_type=MESH),
        ]

    def start(copies):
        for copy in copies:
            copy.start()

    def received(copies):
        for copy in copies:
            copy.wait_recv()

    def sent(copies):
        for copy in copies:
            copy.wait_send()

    def pack(k, ref):
        def body(y, carry):
            for j in range(J):
                KX[k, 1, j, pl.ds(y, 1), :] = ref[j, y + 1, pl.ds(PX, 1), :]
                KX[k, 0, j, pl.ds(y, 1), :] = ref[j, y + 1, pl.ds(PX + X - 1, 1), :]
            return carry
        lax.fori_loop(0, Y, body, 0)

    def unpack_columns(k, ref):
        def body(y, carry):
            for j in range(J):
                ref[j, y + 1, pl.ds(PX + X, 1), :] = LX[k, 1, j, pl.ds(y, 1), :]
                ref[j, y + 1, pl.ds(PX - 1, 1), :] = LX[k, 0, j, pl.ds(y, 1), :]
            return carry
        lax.fori_loop(0, Y, body, 0)

    def unpack_rows(k, ref):
        for j in range(J):
            ref[j, 0, pl.ds(PX, X), :] = LY[k, 0, j]
            ref[j, Y + 1, pl.ds(PX, X), :] = LY[k, 1, j]

    def residual_rows(src, j, y, n, x, w):
        r = [src[j, y + k, pl.ds(PX + x, w), :] for k in range(n + 2)]
        for k in range(n):
            beside = src[j, y + k + 1, pl.ds(PX + x - 1, w), :] + src[j, y + k + 1, pl.ds(PX + x + 1, w), :]
            yield k, r[k + 1], S[j, y + k, pl.ds(x, w), :] + (r[k] + r[k + 2] + beside)

    def relax(src, put, y, n, columns):
        for j in range(J):
            for x, w in columns:
                for k, old, total in residual_rows(src, j, y, n, x, w):
                    put(j, y + k, x, w, 0.2 * old + W[j, y + k, pl.ds(x, w), :] * total)

    def into(ref):
        def put(j, y, x, w, value):
            ref[j, y + 1, pl.ds(PX + x, w), :] = value
        return put

    def into_result(j, y, x, w, value):
        D[y, pl.ds(x, w), pl.ds(j * 128, 128)] = value

    middle_columns = [(x, min(32, X - 8 - x)) for x in range(8, X - 8, 32)]
    edge_columns = [(0, 8), (X - 8, 8)]
    all_columns = [(x, 32) for x in range(0, X, 32)]

    def inner(src, put, columns):
        def body(i, carry):
            relax(src, put, 2 + 4 * i, 4, columns)
            return carry
        lax.fori_loop(0, (Y - 4) // 4, body, 0)

    def outer(src, put):
        def body(i, carry):
            relax(src, put, i * (Y - 2), 2, all_columns)
            return carry
        lax.fori_loop(0, 2, body, 0)

    def each_end(k, coming, src, dst, going):
        for n, low, halo in ((0, 0, 0), (1, Y - 2, Y + 1)):
            coming[1 - n].wait_recv()
            for j in range(J):
                src[j, halo, pl.ds(PX, X), :] = LY[k, n, j]
            relax(src, into(dst), low, 2, all_columns)
            going[n].start()

    def coarse_copies(ref, pieces, base):
        made = []
        for n, (dy, dx, r, nr, c, nc) in enumerate(pieces):
            made.append(pltpu.make_async_remote_copy(
                src_ref=ref.at[:, pl.ds(AGAIN + r, nr), pl.ds(CPX + c, nc), :],
                dst_ref=ref.at[:, pl.ds(AGAIN + r - CY * dy, nr), pl.ds(CPX + c - CX * dx, nc), :],
                send_sem=cs.at[base + n], recv_sem=cr.at[base + n],
                device_id=device(dy, dx), device_id_type=MESH))
        return made

    def corner_copies(which, cells, base):
        return [pltpu.make_async_remote_copy(
            src_ref=KC.at[which, n, :, pl.ds(0, cells), :], dst_ref=LC.at[which, n, :, pl.ds(0, cells), :],
            send_sem=cs.at[base + n], recv_sem=cr.at[base + n],
            device_id=device(dy, dx), device_id_type=MESH) for n, (dy, dx) in enumerate(CORNERS)]

    def pack_corners(which, ref, depth):
        for n, (dy, dx) in enumerate(CORNERS):
            for here, _, c, _, count, place in corner_cells(depth, CY, CX, dy, dx):
                for j in range(J):
                    KC[which, n, j, pl.ds(place, count), :] = ref[j, AGAIN + here, pl.ds(CPX + c, count), :]

    def unpack_corners(which, ref, depth):
        for n, (dy, dx) in enumerate(CORNERS):
            for _, there, _, c, count, place in corner_cells(depth, CY, CX, dy, dx):
                for j in range(J):
                    ref[j, AGAIN + there, pl.ds(CPX + c, count), :] = LC[which, n, j, pl.ds(place, count), :]

    def sides(first, last):
        return [(0, -1, first, last - first, 0, 8), (0, 1, first, last - first, CX - 8, 8)]

    half = DEPTH // 2
    mass_near = coarse_copies(CW, [(-1, 0, 0, half, 0, CX), (1, 0, CY - half, half, 0, CX)], 0)
    mass_far = coarse_copies(
        CW, [(-1, 0, half, DEPTH - half, 0, CX), (1, 0, CY - DEPTH, DEPTH - half, 0, CX)] + sides(0, CY), 2)
    mass_corners = corner_copies(0, 16, 6)
    load_early = coarse_copies(CL, [(-1, 0, 1, DEPTH - 1, 0, CX), (1, 0, CY - DEPTH, DEPTH - 1, 0, CX)], 10)
    load_late = coarse_copies(CL, [(-1, 0, 0, 1, 0, CX), (1, 0, CY - 1, 1, 0, CX)] + sides(0, CY), 12)
    load_corners = corner_copies(1, 16, 16)
    value_copies = coarse_copies(CC, [(-1, 0, 0, AGAIN, 0, CX), (1, 0, CY - AGAIN, AGAIN, 0, CX)] + sides(0, CY), 20)
    value_corners = corner_copies(2, 24, 24)

    rows0, rows1, rows2, rows3 = (rows_copies(0, U), rows_copies(1, V), rows_copies(2, U), rows_copies(3, V))
    cols0, cols1, cols2, cols3 = (columns_copies(0), columns_copies(1), columns_copies(2), columns_copies(3))
    with jax.named_scope("wait_ends"):
        for copy in load_ends + load_tiles:
            copy.wait()
        start(rows0)
    with jax.named_scope("pack0"):
        pack(0, U)
        start(cols0)
    with jax.named_scope("wait_u"):
        for copy in load_u:
            copy.wait()

    with jax.named_scope("wait_d"):
        for copy in load_d:
            copy.wait()

    def fold(ref, j):
        return (ref[j, pl.ds(0, CX, stride=RATIO), :] + ref[j, pl.ds(1, CX, stride=RATIO), :]
                + ref[j, pl.ds(2, CX, stride=RATIO), :] + ref[j, pl.ds(3, CX, stride=RATIO), :])

    def weight_row(cy, carry):
        for j in range(J):
            total = jnp.zeros((X, 128), jnp.float32)
            for r in range(RATIO):
                mass = D[cy * RATIO + r, :, pl.ds(j * 128, 128)]
                total = total + mass
                whole = 4.0 + mass
                D[cy * RATIO + r, :, pl.ds(j * 128, 128)] = whole
                W[j, cy * RATIO + r] = 0.8 / whole
            T[j, 0] = total
            CW[j, AGAIN + cy, pl.ds(CPX, CX), :] = 0.8 / (4.0 + 0.25 * fold(T.at[:, 0], j))
        return carry
    with jax.named_scope("weights"):
        lax.fori_loop(0, CY, weight_row, 0)
        start(mass_near)

    with jax.named_scope("wait_x0"):
        for copy in load_near:
            copy.wait()
        received(cols0)
    with jax.named_scope("unpack0"):
        unpack_columns(0, U)
    with jax.named_scope("outer1"):
        each_end(0, rows0, U, V, rows1)
    with jax.named_scope("wait_s"):
        for copy in load_s:
            copy.wait()
    with jax.named_scope("edges1"):
        inner(U, into(V), edge_columns)
        pack(1, V)
        start(cols1)
        start(mass_far)
        pack_corners(0, CW, DEPTH)
        start(mass_corners)
    with jax.named_scope("middle1"):
        inner(U, into(V), middle_columns)

    sent(rows0)
    with jax.named_scope("middle2"):
        inner(V, into(U), middle_columns)
    with jax.named_scope("wait_x1"):
        received(cols1)
    with jax.named_scope("edges2"):
        unpack_columns(1, V)
        inner(V, into(U), edge_columns)
    with jax.named_scope("outer2"):
        each_end(1, rows1, V, U, rows2)
        pack(2, U)
        start(cols2)

    def defect(cy, columns):
        for j in range(J):
            for x, w in columns:
                total = None
                for k, old, around in residual_rows(U, j, cy * RATIO, RATIO, x, w):
                    term = around - D[cy * RATIO + k, pl.ds(x, w), pl.ds(j * 128, 128)] * old
                    total = term if total is None else total + term
                T[j, cy, pl.ds(x, w), :] = total

    def coarse_load(cy):
        for j in range(J):
            CL[j, AGAIN + cy, pl.ds(CPX, CX), :] = 0.25 * fold(T.at[:, cy], j)

    def defect_middle(cy, carry):
        defect(cy, middle_columns)
        return carry

    def defect_edges(cy, carry):
        defect(cy, edge_columns)
        coarse_load(cy)
        return carry

    def defect_ends(i, carry):
        defect(i * (CY - 1), all_columns)
        coarse_load(i * (CY - 1))
        return carry

    with jax.named_scope("defect_middle"):
        lax.fori_loop(1, CY - 1, defect_middle, 0)
    with jax.named_scope("wait_x2"):
        received(cols2)
    with jax.named_scope("defect_edges"):
        unpack_columns(2, U)
        lax.fori_loop(1, CY - 1, defect_edges, 0)
        start(load_early)
    with jax.named_scope("wait_y2"):
        received(rows2)
    with jax.named_scope("defect_ends"):
        unpack_rows(2, U)
        lax.fori_loop(0, 2, defect_ends, 0)
        start(load_late)
        pack_corners(1, CL, DEPTH)
        start(load_corners)
    with jax.named_scope("wait_mass"):
        received(mass_near + mass_far + mass_corners)
        unpack_corners(0, CW, DEPTH)
    with jax.named_scope("wait_load"):
        received(load_early + load_late + load_corners)
        unpack_corners(1, CL, DEPTH)

    def first(y, carry):
        for j in range(J):
            CA[j, y, pl.ds(CPX - 8, CX + 16), :] = CW[j, y, pl.ds(CPX - 8, CX + 16), :] * CL[j, y, pl.ds(CPX - 8, CX + 16), :]
        return carry

    def coarse_sweep(old, new, reach):
        x0 = CPX - 8 if reach > 0 else CPX
        wide = CX + 2 * (CPX - x0)

        n = 4 if (CY + 2 * reach) % 4 == 0 else 2
        half = wide // 2

        def coarse_rows(i, carry):
            y = AGAIN - reach + n * i
            for j in range(J):
                for x in (x0, x0 + half):
                    r = [old[j, y - 1 + k, pl.ds(x, half), :] for k in range(n + 2)]
                    for k in range(n):
                        beside = old[j, y + k, pl.ds(x - 1, half), :] + old[j, y + k, pl.ds(x + 1, half), :]
                        total = CL[j, y + k, pl.ds(x, half), :] + (r[k] + r[k + 2] + beside)
                        new[j, y + k, pl.ds(x, half), :] = 0.2 * r[k + 1] + CW[j, y + k, pl.ds(x, half), :] * total
            return carry
        lax.fori_loop(0, (CY + 2 * reach) // n, coarse_rows, 0)

    with jax.named_scope("coarse1"):
        lax.fori_loop(AGAIN - DEPTH, AGAIN + CY + DEPTH, first, 0)
        old, new = CA, CB
        for reach in range(DEPTH - 1, -1, -1):
            coarse_sweep(old, CC if reach == 0 else new, reach)
            old, new = new, old
        start(value_copies)
        pack_corners(2, CC, AGAIN)
        start(value_corners)
    with jax.named_scope("wait_value"):
        received(value_copies + value_corners)
        unpack_corners(2, CC, AGAIN)
    with jax.named_scope("coarse2"):
        old, new = CC, CA
        for reach in range(AGAIN - 1, 0, -1):
            coarse_sweep(old, new, reach)
            old, new = new, (CB if new is CA else CA)
        C = old

    def spread(cy):
        for j in range(J):
            cells = C[j, AGAIN + cy, pl.ds(CPX, CX), :]
            for k in range(RATIO):
                E[j, pl.ds(PX + k, CX, stride=RATIO), :] = cells
            E[j, pl.ds(PX - 1, 1), :] = C[j, AGAIN + cy, pl.ds(CPX - 1, 1), :]
            E[j, pl.ds(PX + X, 1), :] = C[j, AGAIN + cy, pl.ds(CPX + CX, 1), :]

    def add_row(y):
        for j in range(J):
            U[j, y] = U[j, y] + E[j]

    sent(rows2)

    def correct(cy, carry):
        spread(cy)
        for r in range(RATIO):
            add_row(1 + cy * RATIO + r)
        return carry

    with jax.named_scope("correct_outer"):
        spread(-1)
        add_row(0)
        spread(CY)
        add_row(Y + 1)
        lax.fori_loop(0, 2, lambda i, carry: correct(i * (CY - 1), carry), 0)
    sent(rows1)
    with jax.named_scope("outer3"):
        for copy, y in zip(rows3, (0, Y - 2)):
            relax(U, into(V), y, 2, all_columns)
            copy.start()
    with jax.named_scope("correct"):
        lax.fori_loop(1, CY - 1, correct, 0)
    with jax.named_scope("sweep3"):
        inner(U, into(V), edge_columns)
        pack(3, V)
        start(cols3)
        inner(U, into(V), middle_columns)
    with jax.named_scope("middle4"):
        inner(V, into_result, middle_columns)
    with jax.named_scope("wait_x3"):
        received(cols3)
    with jax.named_scope("edges4"):
        unpack_columns(3, V)
        inner(V, into_result, edge_columns)
    with jax.named_scope("wait_y3"):
        received(rows3)
    with jax.named_scope("outer4"):
        unpack_rows(3, V)
        outer(V, into_result)
    sent(rows3)
    for copies in (cols0, cols1, cols2, cols3, mass_near, mass_far, mass_corners, load_early, load_late, load_corners,
                   value_copies, value_corners):
        sent(copies)


def store(held, out, sems):
    pieces = sems.shape[0]
    rows = held.shape[0] // pieces
    copies = [pltpu.make_async_copy(held.at[pl.ds(n * rows, rows)], out.at[pl.ds(n * rows, rows)], sems.at[n]) for n in range(pieces)]
    for copy in copies:
        copy.start()
    for copy in copies:
        copy.wait()


def solution(mesh):
    ny, nx = mesh.shape["py"], mesh.shape["px"]

    def local(source_terms, initial_values, absorption):
        Y, X, cases = source_terms.shape
        J = cases // 128
        CY, CX = Y // RATIO, X // RATIO
        f32 = jnp.float32
        fine = pltpu.VMEM((J, Y + 2, X + 2 * PX, 128), f32)
        plain = pltpu.VMEM((J, Y, X, 128), f32)
        coarse = pltpu.VMEM((J, CY + 2 * AGAIN, CX + 2 * CPX, 128), f32)
        dma = pltpu.SemaphoreType.DMA

        def body(*refs):
            kernel(ny, nx, *refs)

        held = pl.pallas_call(
            body,
            out_shape=pltpu.VMEM((Y, X, cases), f32),
            in_specs=[pl.BlockSpec(memory_space=pl.ANY)] * 3,
            out_specs=pl.BlockSpec(memory_space=pltpu.VMEM),
            scratch_shapes=[
                fine, fine, plain, plain, coarse, coarse, coarse, coarse, coarse,
                pltpu.VMEM((J, X + 2 * PX, 128), f32),
                pltpu.VMEM((J, CY, X, 128), f32),
                pltpu.VMEM((4, 2, J, X, 128), f32),
                pltpu.VMEM((4, 2, J, Y, 128), f32),
                pltpu.VMEM((4, 2, J, Y, 128), f32),
                pltpu.VMEM((3, 4, J, 24, 128), f32),
                pltpu.VMEM((3, 4, J, 24, 128), f32),
                dma((18 * J,)),
                dma((4, 2)), dma((4, 2)), dma((4, 2)), dma((4, 2)),
                dma((28,)), dma((28,)),
            ],
            compiler_params=pltpu.CompilerParams(
                collective_id=0, has_side_effects=True, vmem_limit_bytes=52 * 1024 * 1024),
            name="two_grid",
        )(source_terms, initial_values, absorption)
        return pl.pallas_call(
            store,
            out_shape=jax.ShapeDtypeStruct((Y, X, cases), f32),
            in_specs=[pl.BlockSpec(memory_space=pltpu.VMEM)],
            out_specs=pl.BlockSpec(memory_space=pl.ANY),
            scratch_shapes=[dma((8,))],
            compiler_params=pltpu.CompilerParams(vmem_limit_bytes=1024 * 1024),
            name="store",
        )(pltpu.with_memory_space_constraint(held, pltpu.VMEM))

    spec = P("py", "px", None)
    return jax.shard_map(local, mesh=mesh, in_specs=(spec, spec, spec), out_specs=spec, check_vma=False)
```
